32 devices in a mesh: space: 32 (over z, y, x, core), ens: 1.
Axes of the slice: x: 2, y: 2, z: 4, core: 2. Of those that a mesh axis runs over, the one named last changes fastest.
Arguments:
- innovations: bfloat16 [1, 2048, 128, 128], P('ens', 'space'), may hold values from -6 to 6
- block_owner: int32 [2048, 1], P('space'), may hold values from 0 to 31; in each aligned block of 64 rows (0 to 63, 64 to 127, ...) at most 4 rows name the same one
- block_tile: int32 [2048], P('space'), may hold values from 0 to 3
- block_count: int32 [32], P('space'), may hold values from 48 to 64
- obs_row: int32 [2048, 128], P('space'), may hold values from 0 to 6
- obs_col: int32 [2048, 128], P('space'), may hold values from 0 to 14
- offsets: float32 [2048, 2, 128], P('space'), may hold values from 0 to 1
- obs_mask: int32 [2048, 128], P('space'), may hold values 0 or 1
- sigma: float32 [128, 128], P('space'), may hold values from 0.3 to 3
- coupling: float32 [128, 128], replicated, may hold values from -0.5 to 0.5
Outputs:
- gradient: float32 [128, 128, 128], P('ens', 'space')
The draws below stay inside these ranges and needn't reach their ends.
Inputs may be any that keep to these rules, and one draw needn't show every extreme that they name: `block_owner`: among the rows of one device, no owner is named more than 4 times, and one owner is named exactly 4 times in some devices' rows. `block_count`: blocks of a device at positions at or above its count are padding.
All inputs are finite; a program needn't handle non-finite values. No bound on the sum of `obs_mask` on one device may be relied on, other than what follows from the above.
Results may differ from the reference program's by a relative error of at most 0.0095.
Values may be sent and summed in bfloat16 or wider, within the bound.
A program may use at most 64 MiB of HBM per device.

```python
import math
import jax
import jax.numpy as jnp
import numpy as np
from jax import lax

CH = 128
OBS = 128
TH = 8
TW = 16
CELLS = 128
TILE_DEV = 4
TILES = 128
BLK_DEV = 64
BLOCKS = 2048
CAP = 4
MEMBERS = 1
N_SPACE = 32


def with_ends(array, own_key, low, largest):
    place = [jax.random.randint(jax.random.fold_in(own_key, axis), (), 0, length) for axis, length in enumerate(array.shape)]
    main_axis = array.shape.index(max(array.shape))
    beside = place[:main_axis] + [(place[main_axis] + 1) % array.shape[main_axis]] + place[main_axis + 1:]
    return array.at[tuple(place)].set(low).at[tuple(beside)].set(largest)


def levels(own_key, shape, pieces, least, high):
    def one(dim, blocks):
        draws = jax.random.uniform(jax.random.fold_in(jax.random.fold_in(own_key, 6), dim), (blocks,), jnp.float32, least / len(pieces), high / len(pieces))
        return jnp.repeat(jnp.exp(draws), shape[dim] // blocks).reshape((-1,) + (1,) * (len(shape) - dim - 1))

    loudness = one(*pieces[0])
    for cut in pieces[1:]:
        loudness = loudness * one(*cut)
    return loudness


def routed_block(stream_key, own, number, rows, amount, top, reach, skew):
    order = jax.random.permutation(stream_key, amount)
    crowded, common = shares(amount, rows * top, reach, skew, True), shares(amount, rows * top, reach, skew, False)
    places = jnp.arange(amount)

    def named(sizes, rotation):
        used = int((sizes > 0).sum())
        fixed = max(1, used // 4)
        shifted = fixed + (places - fixed + rotation * (used - fixed)) % max(1, amount - fixed)
        return jnp.zeros((amount,), jnp.int32).at[order[jnp.where(places < fixed, places, shifted)]].set(jnp.asarray(sizes, jnp.int32))

    sizes = jnp.where(number % 4 == 0, named(crowded, number // 4), named(common, number - number // 4 - 1))
    mixed = jax.random.permutation(jax.random.fold_in(own, 3), amount)
    donor, taker = mixed[0:amount // 2 * 2:2], mixed[1:amount // 2 * 2:2]
    margin = jnp.minimum(sizes[donor] - 1, reach - sizes[taker]) // 2
    margin = jnp.where((donor == order[0]) | (taker == order[0]) | (sizes[taker] == 0), 0, jnp.maximum(margin, 0))
    shifted = jax.random.randint(jax.random.fold_in(own, 4), (amount // 2,), 0, 1 << 20) % (margin + 1)
    sizes = sizes.at[donor].add(-shifted).at[taker].add(shifted)
    labels = jnp.searchsorted(jnp.cumsum(sizes), jnp.arange(rows * top), side="right").astype(jnp.int32)
    grid = labels.reshape(top, rows).T
    grid = grid[jax.random.permutation(jax.random.fold_in(own, 1), rows)]
    rotation = jax.random.randint(jax.random.fold_in(own, 2), (rows, 1), 0, top)
    return jnp.take_along_axis(grid, (jnp.arange(top)[None, :] + rotation) % top, axis=1)


def shares(amount, total, bound, lean, full):
    loads = [(1 << 20) // math.isqrt(rank ** lean) + 1 for rank in range(1, amount + 1)]
    largest = bound if full else min(bound, max(-(-total // amount), total * loads[0] // sum(loads)))
    least = 1 if total - largest >= amount - 1 else 0
    holding, rest = [largest] + [least] * (amount - 1), total - largest - least * (amount - 1)
    while rest > 0:
        free = [i for i in range(1, amount) if holding[i] < largest] or [i for i in range(1, amount) if holding[i] < bound]
        pool, remaining = sum([loads[i] for i in free]), rest
        for i in free:
            extra = min(bound - holding[i], max(1, remaining * loads[i] // pool), rest)
            holding[i] = holding[i] + extra
            rest = rest - extra
    return np.array(holding)


def noise(own_key, extent, width, bound, cuts=(), kind=jnp.bfloat16):
    array = jax.random.normal(own_key, extent, jnp.float32) * width
    if len(cuts) > 0:
        array = levels(own_key, extent, cuts, -0.22, 0.18) * array
    return jnp.clip(array, min=-bound, max=bound).astype(kind)


def setup_inputs(seed: int = 0) -> dict:
    keys = jax.random.split(jax.random.key(seed), 11)
    innovations = noise(keys[0], (MEMBERS, BLOCKS, OBS, CH), 1.0, 6.0, ((1, 32),))
    block_owner_keys = jax.random.split(jax.random.fold_in(keys[1], 1), BLOCKS // BLK_DEV)
    block_owner_turns = jax.random.permutation(jax.random.fold_in(keys[1], 3), BLOCKS // BLK_DEV)
    block_owner = jax.vmap(lambda own, number: routed_block(jax.random.fold_in(keys[1], 2), own, number, BLK_DEV, N_SPACE, 1, CAP, 2))(block_owner_keys, block_owner_turns).reshape((BLOCKS, 1))
    block_tile = with_ends(jax.random.randint(keys[2], (BLOCKS,), 0, TILE_DEV), jax.random.fold_in(keys[2], 1), 0, TILE_DEV - 1).astype(jnp.int32)
    block_count = with_ends(jax.random.randint(keys[3], (N_SPACE,), 3 * BLK_DEV // 4, BLK_DEV + 1), jax.random.fold_in(keys[3], 1), 3 * BLK_DEV // 4, BLK_DEV).astype(jnp.int32)
    obs_row = with_ends(jax.random.randint(keys[4], (BLOCKS, OBS), 0, TH - 1), jax.random.fold_in(keys[4], 1), 0, (TH - 1) - 1).astype(jnp.int32)
    obs_col = with_ends(jax.random.randint(keys[5], (BLOCKS, OBS), 0, TW - 1), jax.random.fold_in(keys[5], 1), 0, (TW - 1) - 1).astype(jnp.int32)
    offsets = jnp.clip(1.0 * jax.random.uniform(keys[6], (BLOCKS, 2, OBS), jnp.float32) ** levels(keys[6], (BLOCKS, 2, OBS), ((0, 32),), -0.2, 0.2), 0.0, 1.0)
    obs_mask = with_ends((jax.random.randint(keys[7], (BLOCKS, OBS), 0, 4) < 3).astype(jnp.int32), jax.random.fold_in(keys[7], 1), 0, 1)
    sigma = jnp.clip(jnp.exp(math.log(3.0) - 2.3025851 * jax.random.uniform(keys[8], (TILES, CH), jnp.float32) ** levels(keys[8], (TILES, CH), ((0, 32),), -0.2, 0.2)), 0.3, 3.0)
    coupling = noise(keys[9], (CELLS, CELLS), CELLS ** -0.5, 0.5, (), jnp.float32)
    return {"innovations": innovations, "block_owner": block_owner, "block_tile": block_tile, "block_count": block_count, "obs_row": obs_row, "obs_col": obs_col, "offsets": offsets, "obs_mask": obs_mask, "sigma": sigma, "coupling": coupling}


def reference(innovations, block_owner, block_tile, block_count, obs_row, obs_col, offsets, obs_mask, sigma, coupling):
    blocks = block_owner.shape[0]
    per_device = blocks // block_count.shape[0]
    position = jnp.arange(blocks, dtype=jnp.int32)
    alive = (position % per_device) < block_count[position // per_device]
    live = obs_mask.astype(jnp.float32) * alive[:, None].astype(jnp.float32)
    row_frac = offsets[:, 0, :]
    col_frac = offsets[:, 1, :]
    tile = block_owner[:, 0] * TILE_DEV + block_tile
    summed = jnp.sum(innovations.astype(jnp.float32), axis=0).reshape(-1, CH)
    total = jnp.zeros((TILES * CELLS, CH), jnp.float32)
    for down in (0, 1):
        for right in (0, 1):
            row_part = row_frac if down == 1 else 1.0 - row_frac
            col_part = col_frac if right == 1 else 1.0 - col_frac
            rounded = (row_part * col_part * live).astype(jnp.bfloat16)
            rounded = lax.optimization_barrier(rounded).astype(jnp.float32)
            target = tile[:, None] * CELLS + (obs_row + down) * TW + obs_col + right
            total = total.at[target.reshape(-1)].add(summed * rounded.reshape(-1, 1))
    mean = total.reshape(TILES, CELLS, CH) / MEMBERS
    coupled = jnp.einsum("ck,tkh->cth", coupling, mean, precision=lax.Precision.HIGHEST)
    return sigma[None, :, :] * (jnp.transpose(mean, (1, 0, 2)) + coupled)
```

```python
import functools

import jax
import jax.numpy as jnp
from jax import lax
from jax.experimental import pallas as pl
from jax.experimental.pallas import tpu as pltpu
from jax.sharding import PartitionSpec as P

TW = 16
GROUP = 4
STREAMS = 6
ROTATED = 3


MESH = pl.DeviceIdType.MESH


def partial_kernel(
    cells, owner_ref, tile_ref, count_ref, innov_ref, row_ref, col_ref, off_ref, mask_ref,
    send_ref, keep_ref, acc, packed, base_s, weight_s, sem,
):
    blocks, obs, width = innov_ref.shape
    half, rows, _ = packed.shape
    me = lax.axis_index("space")

    def clear(i, carry):
        acc[pl.ds(pl.multiple_of(i * rows, rows), rows), :] = jnp.zeros((rows, width), jnp.float32)
        return carry

    lax.fori_loop(0, 2 * half, clear, 0)
    alive = lax.broadcasted_iota(jnp.int32, (blocks, obs), 0) < count_ref[0]
    live = jnp.where(alive, mask_ref[...].astype(jnp.float32), 0.0)
    row_frac = off_ref[:, 0, :]
    col_frac = off_ref[:, 1, :]
    base_s[...] = row_ref[...] * TW + col_ref[...]
    corners = (
        (1.0 - row_frac) * (1.0 - col_frac),
        (1.0 - row_frac) * col_frac,
        row_frac * (1.0 - col_frac),
        row_frac * col_frac,
    )
    for k, corner in enumerate(corners):
        weight_s[k, :, :] = (corner * live).astype(jnp.bfloat16).astype(jnp.float32)
    cell = lax.broadcasted_iota(jnp.int32, (cells, obs), 0)

    def accumulate(turn, carry):
        sums = []
        for g in range(GROUP):
            b = turn * GROUP + g
            away = cell - base_s[pl.ds(b, 1), :]
            table = jnp.zeros((cells, obs), jnp.float32)
            for k, step in enumerate((0, 1, TW, TW + 1)):
                table = jnp.where(away == step, weight_s[k, pl.ds(b, 1), :], table)
            sums.append(
                jnp.dot(table.astype(jnp.bfloat16), innov_ref[b], preferred_element_type=jnp.float32)
            )
        for g in range(GROUP):
            b = turn * GROUP + g
            slot = lax.bitwise_xor(owner_ref[b], me)
            place = (slot % 2) * half + slot // 2
            at = pl.ds(pl.multiple_of(place * rows + tile_ref[b] * cells, cells), cells)
            acc[at, :] += sums[g]
        return carry

    lax.fori_loop(0, blocks // GROUP, accumulate, 0)

    keep = pltpu.make_async_copy(acc.at[pl.ds(0, half * rows), :], keep_ref, sem.at[0])
    keep.start()

    def pack(i, carry):
        packed[i] = acc[pl.ds(pl.multiple_of((half + i) * rows, rows), rows), :].astype(jnp.bfloat16)
        return carry

    lax.fori_loop(0, half, pack, 0)
    out = pltpu.make_async_copy(packed, send_ref, sem.at[1])
    out.start()
    out.wait()
    keep.wait()


def spread(index, places):
    total = 0
    for j, place in enumerate(places):
        total = total + ((index // (1 << j)) % 2) * (1 << place)
    return total


def plans(bits, rows):
    unit = 16
    count = min(STREAMS, rows // unit)
    edges = [rows // unit * i // count * unit for i in range(count + 1)]
    head = list(range(1, min(1 + ROTATED, bits)))
    tail = list(range(1 + len(head), bits))
    made = []
    for i in range(count):
        turn = i % max(1, len(head))
        made.append((edges[i], edges[i + 1], [0] + head[turn:] + head[:turn] + tail))
    return made


def scatter_kernel(bits, streams, send_ref, keep_ref, out_ref, keep, *scratch):
    count = len(streams)
    recv = [scratch[i * bits : (i + 1) * bits] for i in range(count)]
    sent = [scratch[(count + i) * bits : (count + i + 1) * bits] for i in range(count)]
    send_sem, recv_sem, keep_sem = scratch[2 * count * bits :]
    me = lax.axis_index("space")
    rows = out_ref.shape[0]

    def partner(bit):
        return me + (1 << bit) - 2 * (1 << bit) * ((me // (1 << bit)) % 2)

    barrier = pltpu.get_barrier_semaphore()
    for bit in range(bits):
        pl.semaphore_signal(barrier, inc=1, device_id={"space": partner(bit)}, device_id_type=MESH)
    load = pltpu.make_async_copy(keep_ref, keep, keep_sem)
    load.start()
    pl.semaphore_wait(barrier, bits)

    def copy(i, stage):
        low, high, order = streams[i]
        source = send_ref.at[:, pl.ds(low, high - low), :] if stage == 0 else sent[i][stage]
        return pltpu.make_async_remote_copy(
            src_ref=source,
            dst_ref=recv[i][stage],
            send_sem=send_sem.at[i * bits + stage],
            recv_sem=recv_sem.at[i * bits + stage],
            device_id={"space": partner(order[stage])},
            device_id_type=MESH,
        )

    copies = {}
    for i in range(count):
        copies[i, 0] = copy(i, 0)
        copies[i, 0].start()
    load.wait()
    for stage in range(bits):
        for i, (low, high, order) in enumerate(streams):
            copies[i, stage].wait_recv()
            got = recv[i][stage]
            left = sorted(order[stage + 1 :])
            if not left:
                out_ref[pl.ds(low, high - low), :] = (
                    keep[pl.ds(low, high - low), :] + got[0].astype(jnp.float32)
                )
                continue
            bit = order[stage + 1]
            rest = [b for b in left if b != bit]
            seat = left.index(bit)
            seats = [j for j in range(len(left)) if j != seat]

            def away(r, carry):
                slot = spread(r, [b - 1 for b in rest]) + (1 << (bit - 1))
                at = pl.ds(pl.multiple_of(slot * rows + low, 16), high - low)
                total = keep[at, :] + got[spread(r, seats) + (1 << seat)].astype(jnp.float32)
                sent[i][stage + 1][r] = total.astype(jnp.bfloat16)
                return carry

            def stay(r, carry):
                slot = spread(r, [b - 1 for b in rest])
                at = pl.ds(pl.multiple_of(slot * rows + low, 16), high - low)
                keep[at, :] += got[spread(r, seats)].astype(jnp.float32)
                return carry

            lax.fori_loop(0, 1 << len(rest), away, 0)
            copies[i, stage + 1] = copy(i, stage + 1)
            copies[i, stage + 1].start()
            lax.fori_loop(0, 1 << len(rest), stay, 0)
    for made in copies.values():
        made.wait_send()


def local_sums(
    innovations, block_owner, block_tile, block_count, obs_row, obs_col, offsets, obs_mask, tile_local, cells, peers
):
    blocks, obs, width = innovations.shape
    half, rows = peers // 2, tile_local * cells
    smem = pl.BlockSpec(memory_space=pltpu.SMEM)
    vmem = pl.BlockSpec(memory_space=pltpu.VMEM)
    hbm = pl.BlockSpec(memory_space=pl.ANY)
    return pl.pallas_call(
        functools.partial(partial_kernel, cells),
        out_shape=(
            jax.ShapeDtypeStruct((half, rows, width), jnp.bfloat16),
            jax.ShapeDtypeStruct((half * rows, width), jnp.float32),
        ),
        in_specs=[smem] * 3 + [vmem] * 5,
        out_specs=(hbm, hbm),
        scratch_shapes=[
            pltpu.VMEM((2 * half * rows, width), jnp.float32),
            pltpu.VMEM((half, rows, width), jnp.bfloat16),
            pltpu.VMEM((blocks, obs), jnp.int32),
            pltpu.VMEM((4, blocks, obs), jnp.float32),
            pltpu.SemaphoreType.DMA((2,)),
        ],
        compiler_params=pltpu.CompilerParams(vmem_limit_bytes=56 << 20),
    )(block_owner, block_tile, block_count, innovations, obs_row, obs_col, offsets, obs_mask)


def scatter_sums(send, keep, rows, width, peers):
    bits = peers.bit_length() - 1
    streams = plans(bits, rows)
    hbm = pl.BlockSpec(memory_space=pl.ANY)
    held = [
        pltpu.VMEM((1 << (bits - 1 - stage), high - low, width), jnp.bfloat16)
        for low, high, _ in streams
        for stage in range(bits)
    ]
    outgoing = [
        pltpu.VMEM((1 << (bits - 1 - stage) if stage else 1, high - low, width), jnp.bfloat16)
        for low, high, _ in streams
        for stage in range(bits)
    ]
    return pl.pallas_call(
        functools.partial(scatter_kernel, bits, streams),
        out_shape=jax.ShapeDtypeStruct((rows, width), jnp.float32),
        in_specs=[hbm, hbm],
        out_specs=pl.BlockSpec(memory_space=pltpu.VMEM),
        scratch_shapes=[pltpu.VMEM((peers // 2 * rows, width), jnp.float32)]
        + held
        + outgoing
        + [
            pltpu.SemaphoreType.DMA((len(streams) * bits,)),
            pltpu.SemaphoreType.DMA((len(streams) * bits,)),
            pltpu.SemaphoreType.DMA,
        ],
        compiler_params=pltpu.CompilerParams(
            collective_id=0, has_side_effects=True, vmem_limit_bytes=60 << 20
        ),
    )(send, keep)


def on_device(
    innovations, block_owner, block_tile, block_count, obs_row, obs_col, offsets, obs_mask, sigma, coupling
):
    peers = lax.axis_size("space")
    ens_count = lax.axis_size("ens")
    members = ens_count * innovations.shape[0]
    tile_local, width = sigma.shape
    cells = coupling.shape[0]
    values = innovations[0]
    send, keep = local_sums(
        values, block_owner[:, 0], block_tile, block_count, obs_row, obs_col, offsets, obs_mask,
        tile_local, cells, peers,
    )
    totals = scatter_sums(send, keep, tile_local * cells, width, peers)
    totals = totals.reshape(tile_local, cells, width)
    share = cells // ens_count
    if ens_count > 1:
        totals = lax.psum(totals.astype(jnp.bfloat16), "ens").astype(jnp.float32)
    first = lax.axis_index("ens") * share
    coupling_rows = lax.dynamic_slice_in_dim(coupling, first, share, 0)
    own = lax.dynamic_slice_in_dim(totals, first, share, 1)
    coupled = jnp.einsum("ck,tkh->cth", coupling_rows, totals, precision=lax.Precision.HIGHEST)
    return sigma[None, :, :] * (jnp.transpose(own, (1, 0, 2)) + coupled) / members


def solution(mesh):
    in_specs = (
        P("ens", "space", None, None),
        P("space", None),
        P("space"),
        P("space"),
        P("space", None),
        P("space", None),
        P("space", None, None),
        P("space", None),
        P("space", None),
        P(),
    )
    out_specs = P("ens", "space", None)
    return jax.shard_map(
        on_device, mesh=mesh, in_specs=in_specs, out_specs=out_specs, check_vma=False
    )
```

```python
import functools

import jax
import jax.numpy as jnp
from jax import lax
from jax.experimental import pallas as pl
from jax.experimental.pallas import tpu as pltpu
from jax.sharding import PartitionSpec as P

TW = 16
GROUP = 4
STREAMS = 6
ROTATED = 3


MESH = pl.DeviceIdType.MESH


def partial_kernel(
    cells, owner_ref, tile_ref, count_hbm, innov_hbm, row_ref, col_ref, off_ref, mask_ref,
    send_ref, keep_ref, acc, innov_ref, count_ref, base_s, weight_s, sem, count_sem,
):
    blocks, obs, width = innov_ref.shape
    half, rows, _ = send_ref.shape
    me = lax.axis_index("space")
    load = pltpu.make_async_copy(innov_hbm, innov_ref, sem)
    load.start()
    number = pltpu.make_async_copy(count_hbm, count_ref, count_sem)
    number.start()

    def clear(i, carry):
        acc[pl.ds(pl.multiple_of(i * rows, rows), rows), :] = jnp.zeros((rows, width), jnp.float32)
        return carry

    lax.fori_loop(0, 2 * half, clear, 0)
    number.wait()
    alive = lax.broadcasted_iota(jnp.int32, (blocks, obs), 0) < count_ref[0]
    live = jnp.where(alive, mask_ref[...].astype(jnp.float32), 0.0)
    row_frac = off_ref[:, 0, :]
    col_frac = off_ref[:, 1, :]
    base_s[...] = row_ref[...] * TW + col_ref[...]
    corners = (
        (1.0 - row_frac) * (1.0 - col_frac),
        (1.0 - row_frac) * col_frac,
        row_frac * (1.0 - col_frac),
        row_frac * col_frac,
    )
    for k, corner in enumerate(corners):
        weight_s[k, :, :] = (corner * live).astype(jnp.bfloat16).astype(jnp.float32)
    cell = lax.broadcasted_iota(jnp.int32, (cells, obs), 0)

    def accumulate(turn, carry):
        sums = []
        for g in range(GROUP):
            b = turn * GROUP + g
            away = cell - base_s[pl.ds(b, 1), :]
            table = jnp.zeros((cells, obs), jnp.float32)
            for k, step in enumerate((0, 1, TW, TW + 1)):
                table = jnp.where(away == step, weight_s[k, pl.ds(b, 1), :], table)
            sums.append(
                jnp.dot(table.astype(jnp.bfloat16), innov_ref[b], preferred_element_type=jnp.float32)
            )
        for g in range(GROUP):
            b = turn * GROUP + g
            slot = lax.bitwise_xor(owner_ref[b], me)
            place = (slot % 2) * half + slot // 2
            at = pl.ds(pl.multiple_of(place * rows + tile_ref[b] * cells, cells), cells)
            acc[at, :] += sums[g]
        return carry

    load.wait()
    lax.fori_loop(0, blocks // GROUP, accumulate, 0)

    def pack(i, carry):
        own = pl.ds(pl.multiple_of(i * rows, rows), rows)
        send_ref[i] = acc[pl.ds(pl.multiple_of((half + i) * rows, rows), rows), :].astype(jnp.bfloat16)
        keep_ref[own, :] = acc[own, :].astype(keep_ref.dtype)
        return carry

    lax.fori_loop(0, half, pack, 0)


def spread(index, places):
    total = 0
    for j, place in enumerate(places):
        total = total + ((index // (1 << j)) % 2) * (1 << place)
    return total


def plans(bits, rows):
    unit = 16
    count = min(STREAMS, rows // unit)
    edges = [rows // unit * i // count * unit for i in range(count + 1)]
    head = list(range(1, min(1 + ROTATED, bits)))
    tail = list(range(1 + len(head), bits))
    made = []
    for i in range(count):
        turn = i % max(1, len(head))
        made.append((edges[i], edges[i + 1], [0] + head[turn:] + head[:turn] + tail))
    return made


def scatter_kernel(bits, streams, tail, send_ref, keep_ref, *rest):
    if tail:
        sigma_ref, coupling_ref, *rest = rest
    out_ref, *rest = rest
    count = len(streams)
    recv, rest = [rest[i * bits : (i + 1) * bits] for i in range(count)], rest[count * bits :]
    sent, rest = [rest[i * (bits - 1) : (i + 1) * (bits - 1)] for i in range(count)], rest[count * (bits - 1) :]
    kept, (total_ref, send_sem, recv_sem) = rest[:count], rest[count:]
    me = lax.axis_index("space")
    rows, width = total_ref.shape

    def partner(bit):
        return me + (1 << bit) - 2 * (1 << bit) * ((me // (1 << bit)) % 2)

    barrier = pltpu.get_barrier_semaphore()
    for bit in range(bits):
        pl.semaphore_signal(barrier, inc=1, device_id={"space": partner(bit)}, device_id_type=MESH)
    pl.semaphore_wait(barrier, bits)

    def copy(i, stage):
        low, high, order = streams[i]
        source = send_ref.at[:, pl.ds(low, high - low), :] if stage == 0 else sent[i][stage - 1]
        return pltpu.make_async_remote_copy(
            src_ref=source,
            dst_ref=recv[i][stage],
            send_sem=send_sem.at[i * bits + stage],
            recv_sem=recv_sem.at[i * bits + stage],
            device_id={"space": partner(order[stage])},
            device_id_type=MESH,
        )

    copies = {}
    for i in range(count):
        copies[i, 0] = copy(i, 0)
        copies[i, 0].start()
    for stage in range(bits):
        for i, (low, high, order) in enumerate(streams):
            copies[i, stage].wait_recv()
            got = recv[i][stage]
            left = sorted(order[stage + 1 :])
            held = sorted(order[2:])
            if not left:
                total_ref[pl.ds(low, high - low), :] = kept[i][0] + got[0].astype(jnp.float32)
                continue
            bit = order[stage + 1]
            others = [b for b in left if b != bit]
            seats = [left.index(b) for b in others]
            seat = left.index(bit)

            def have(r, upper):
                if stage == 0:
                    slot = spread(r, [b - 1 for b in others]) + upper * (1 << (bit - 1))
                    return keep_ref[pl.ds(pl.multiple_of(slot * rows + low, 16), high - low), :].astype(jnp.float32)
                return kept[i][spread(r, [held.index(b) for b in others]) + upper * (1 << held.index(bit))]

            def away(r, carry):
                total = have(r, 1) + got[spread(r, seats) + (1 << seat)].astype(jnp.float32)
                sent[i][stage][r] = total.astype(jnp.bfloat16)
                return carry

            def stay(r, carry):
                kept[i][spread(r, [held.index(b) for b in others])] = have(r, 0) + got[spread(r, seats)].astype(
                    jnp.float32
                )
                return carry

            lax.fori_loop(0, 1 << len(others), away, 0)
            copies[i, stage + 1] = copy(i, stage + 1)
            copies[i, stage + 1].start()
            lax.fori_loop(0, 1 << len(others), stay, 0)
    if tail:
        cells, tiles, _ = out_ref.shape
        mean = [total_ref[pl.ds(t * cells, cells), :] for t in range(tiles)]
        coupled = jnp.dot(
            coupling_ref[...], jnp.concatenate(mean, axis=1),
            precision=lax.Precision.HIGHEST, preferred_element_type=jnp.float32,
        )
        for t in range(tiles):
            out_ref[:, t, :] = sigma_ref[pl.ds(t, 1), :] * (mean[t] + coupled[:, t * width : (t + 1) * width])
    else:
        out_ref[...] = total_ref[...]
    for made in copies.values():
        made.wait_send()


def local_sums(
    innovations, block_owner, block_tile, block_count, obs_row, obs_col, offsets, obs_mask, tile_local, cells, peers
):
    blocks, obs, width = innovations.shape
    half, rows = peers // 2, tile_local * cells
    kind = jnp.float32 if peers * rows * width <= 1 << 22 else jnp.bfloat16
    smem = pl.BlockSpec(memory_space=pltpu.SMEM)
    vmem = pl.BlockSpec(memory_space=pltpu.VMEM)
    hbm = pl.BlockSpec(memory_space=pltpu.HBM)
    return pl.pallas_call(
        functools.partial(partial_kernel, cells),
        out_shape=(
            pltpu.VMEM((half, rows, width), jnp.bfloat16),
            pltpu.VMEM((half * rows, width), kind),
        ),
        in_specs=[smem] * 2 + [hbm, hbm] + [vmem] * 4,
        out_specs=(vmem, vmem),
        scratch_shapes=[
            pltpu.VMEM((2 * half * rows, width), jnp.float32),
            pltpu.VMEM((blocks, obs, width), jnp.bfloat16),
            pltpu.SMEM((1,), jnp.int32),
            pltpu.VMEM((blocks, obs), jnp.int32),
            pltpu.VMEM((4, blocks, obs), jnp.float32),
            pltpu.SemaphoreType.DMA,
            pltpu.SemaphoreType.DMA,
        ],
        compiler_params=pltpu.CompilerParams(vmem_limit_bytes=limit(peers, rows, width, -3, 62)),
    )(block_owner, block_tile, block_count, innovations, obs_row, obs_col, offsets, obs_mask)


def limit(peers, rows, width, whole, more):
    return peers * rows * width * whole + (more << 20)


def scatter_sums(send, keep, sigma, coupling, tile_local, cells, peers, tail):
    bits = peers.bit_length() - 1
    width, rows = sigma.shape[1], tile_local * cells
    streams = plans(bits, rows)
    vmem = pl.BlockSpec(memory_space=pltpu.VMEM)

    def room(first, kind):
        return [
            pltpu.VMEM((1 << (bits - 1 - stage), high - low, width), kind)
            for low, high, _ in streams
            for stage in range(first, bits)
        ]

    kept = [pltpu.VMEM((1 << (bits - 2), high - low, width), jnp.float32) for low, high, _ in streams]
    shape = (cells, tile_local, width) if tail else (rows, width)
    return pl.pallas_call(
        functools.partial(scatter_kernel, bits, streams, tail),
        out_shape=jax.ShapeDtypeStruct(shape, jnp.float32),
        in_specs=[vmem] * (4 if tail else 2),
        out_specs=vmem,
        scratch_shapes=room(0, jnp.bfloat16)
        + room(1, jnp.bfloat16)
        + kept
        + [
            pltpu.VMEM((rows, width), jnp.float32),
            pltpu.SemaphoreType.DMA((len(streams) * bits,)),
            pltpu.SemaphoreType.DMA((len(streams) * bits,)),
        ],
        compiler_params=pltpu.CompilerParams(
            collective_id=0, has_side_effects=True, vmem_limit_bytes=limit(peers, rows, width, 4, 4)
        ),
    )(send, keep, *((sigma, coupling) if tail else ()))


def on_device(
    innovations, block_owner, block_tile, block_count, obs_row, obs_col, offsets, obs_mask, sigma, coupling
):
    peers = lax.axis_size("space")
    ens_count = lax.axis_size("ens")
    members = ens_count * innovations.shape[0]
    tile_local, width = sigma.shape
    cells = coupling.shape[0]
    values = innovations[0]
    send, keep = local_sums(
        values, block_owner[:, 0], block_tile, block_count, obs_row, obs_col, offsets, obs_mask,
        tile_local, cells, peers,
    )
    totals = scatter_sums(send, keep, sigma, coupling, tile_local, cells, peers, members == 1)
    if members == 1:
        return totals
    totals = totals.reshape(tile_local, cells, width)
    share = cells // ens_count
    if ens_count > 1:
        totals = lax.psum(totals.astype(jnp.bfloat16), "ens").astype(jnp.float32)
    first = lax.axis_index("ens") * share
    coupling_rows = lax.dynamic_slice_in_dim(coupling, first, share, 0)
    own = lax.dynamic_slice_in_dim(totals, first, share, 1)
    coupled = jnp.einsum("ck,tkh->cth", coupling_rows, totals, precision=lax.Precision.HIGHEST)
    return sigma[None, :, :] * (jnp.transpose(own, (1, 0, 2)) + coupled) / members


def solution(mesh):
    in_specs = (
        P("ens", "space", None, None),
        P("space", None),
        P("space"),
        P("space"),
        P("space", None),
        P("space", None),
        P("space", None, None),
        P("space", None),
        P("space", None),
        P(),
    )
    out_specs = P("ens", "space", None)
    return jax.shard_map(
        on_device, mesh=mesh, in_specs=in_specs, out_specs=out_specs, check_vma=False
    )
```

```python
import functools

import jax
import jax.numpy as jnp
from jax import lax
from jax.experimental import pallas as pl
from jax.experimental.pallas import tpu as pltpu
from jax.sharding import PartitionSpec as P

TW = 16
GROUP = 16
PIECES = (1, 1, 1)
SHARES = (1, 1, 1)


MESH = pl.DeviceIdType.MESH


def partial_kernel(
    cells, owner_ref, tile_ref, count_hbm, innov_hbm, row_ref, col_ref, off_ref, mask_ref,
    send_ref, keep_ref, acc, innov_ref, count_ref, base_s, weight_s, sem, count_sem,
):
    blocks, obs, width = innov_ref.shape
    half, rows, _ = send_ref.shape
    me = lax.axis_index("space")
    load = pltpu.make_async_copy(innov_hbm, innov_ref, sem)
    load.start()
    number = pltpu.make_async_copy(count_hbm, count_ref, count_sem)
    number.start()

    def clear(i, carry):
        acc[pl.ds(pl.multiple_of(i * rows, rows), rows), :] = jnp.zeros((rows, width), jnp.float32)
        return carry

    lax.fori_loop(0, 2 * half, clear, 0)
    number.wait()
    alive = lax.broadcasted_iota(jnp.int32, (blocks, obs), 0) < count_ref[0]
    live = jnp.where(alive, mask_ref[...].astype(jnp.float32), 0.0)
    row_frac = off_ref[:, 0, :]
    col_frac = off_ref[:, 1, :]
    base_s[...] = row_ref[...] * TW + col_ref[...]
    corners = (
        (1.0 - row_frac) * (1.0 - col_frac),
        (1.0 - row_frac) * col_frac,
        row_frac * (1.0 - col_frac),
        row_frac * col_frac,
    )
    for k, corner in enumerate(corners):
        weight_s[k, :, :] = (corner * live).astype(jnp.bfloat16).astype(jnp.float32)
    cell = lax.broadcasted_iota(jnp.int32, (cells, obs), 0)

    def accumulate(turn, carry):
        sums = []
        for g in range(GROUP):
            b = turn * GROUP + g
            away = cell - base_s[pl.ds(b, 1), :]
            table = jnp.zeros((cells, obs), jnp.float32)
            for k, step in enumerate((0, 1, TW, TW + 1)):
                table = jnp.where(away == step, weight_s[k, pl.ds(b, 1), :], table)
            sums.append(
                jnp.dot(table.astype(jnp.bfloat16), innov_ref[b], preferred_element_type=jnp.float32)
            )
        for g in range(GROUP):
            b = turn * GROUP + g
            slot = lax.bitwise_xor(owner_ref[b], me)
            place = (slot % 2) * half + slot // 2
            at = pl.ds(pl.multiple_of(place * rows + tile_ref[b] * cells, cells), cells)
            acc[at, :] += sums[g]
        return carry

    load.wait()
    lax.fori_loop(0, blocks // GROUP, accumulate, 0)

    def pack(i, carry):
        own = pl.ds(pl.multiple_of(i * rows, rows), rows)
        send_ref[i] = acc[pl.ds(pl.multiple_of((half + i) * rows, rows), rows), :].astype(jnp.bfloat16)
        keep_ref[own, :] = acc[own, :].astype(keep_ref.dtype)
        return carry

    lax.fori_loop(0, half, pack, 0)


def spread(index, places):
    total = 0
    for j, place in enumerate(places):
        total = total + ((index // (1 << j)) % 2) * (1 << place)
    return total


def plans(bits, rows):
    unit = 16
    head = list(range(1, min(1 + len(SHARES), bits)))
    tail = list(range(1 + len(head), bits))
    sizes = [(piece * SHARES[turn], turn) for piece in PIECES for turn in range(len(head))]
    whole = sum(size for size, _ in sizes)
    made, done, low = [], 0, 0
    for size, turn in sizes:
        done += size
        high = (2 * done * (rows // unit) + whole) // (2 * whole) * unit
        if high > low:
            made.append((low, high, [0] + head[turn:] + head[:turn] + tail))
        low = high
    return made


def scatter_kernel(bits, streams, tail, send_ref, keep_ref, *rest):
    if tail:
        sigma_ref, coupling_ref, *rest = rest
    out_ref, *rest = rest
    count = len(streams)
    recv, rest = [rest[i * bits : (i + 1) * bits] for i in range(count)], rest[count * bits :]
    sent, rest = [rest[i * (bits - 1) : (i + 1) * (bits - 1)] for i in range(count)], rest[count * (bits - 1) :]
    kept, (total_ref, send_sem, recv_sem) = rest[:count], rest[count:]
    me = lax.axis_index("space")
    rows, width = total_ref.shape

    def partner(bit):
        return me + (1 << bit) - 2 * (1 << bit) * ((me // (1 << bit)) % 2)

    barrier = pltpu.get_barrier_semaphore()
    for bit in range(bits):
        pl.semaphore_signal(barrier, inc=1, device_id={"space": partner(bit)}, device_id_type=MESH)
    pl.semaphore_wait(barrier, bits)

    def copy(i, stage):
        low, high, order = streams[i]
        source = send_ref.at[:, pl.ds(low, high - low), :] if stage == 0 else sent[i][stage - 1]
        return pltpu.make_async_remote_copy(
            src_ref=source,
            dst_ref=recv[i][stage],
            send_sem=send_sem.at[i * bits + stage],
            recv_sem=recv_sem.at[i * bits + stage],
            device_id={"space": partner(order[stage])},
            device_id_type=MESH,
        )

    copies = {}
    for i in range(count):
        copies[i, 0] = copy(i, 0)
        copies[i, 0].start()
    for stage in range(bits):
        for i, (low, high, order) in enumerate(streams):
            copies[i, stage].wait_recv()
            got = recv[i][stage]
            left = sorted(order[stage + 1 :])
            held = sorted(order[2:])
            if not left:
                total_ref[pl.ds(low, high - low), :] = kept[i][0] + got[0].astype(jnp.float32)
                continue
            bit = order[stage + 1]
            others = [b for b in left if b != bit]
            seats = [left.index(b) for b in others]
            seat = left.index(bit)

            def have(r, upper):
                if stage == 0:
                    slot = spread(r, [b - 1 for b in others]) + upper * (1 << (bit - 1))
                    return keep_ref[pl.ds(pl.multiple_of(slot * rows + low, 16), high - low), :].astype(jnp.float32)
                return kept[i][spread(r, [held.index(b) for b in others]) + upper * (1 << held.index(bit))]

            def away(r, carry):
                total = have(r, 1) + got[spread(r, seats) + (1 << seat)].astype(jnp.float32)
                sent[i][stage][r] = total.astype(jnp.bfloat16)
                return carry

            def stay(r, carry):
                kept[i][spread(r, [held.index(b) for b in others])] = have(r, 0) + got[spread(r, seats)].astype(
                    jnp.float32
                )
                return carry

            lax.fori_loop(0, 1 << len(others), away, 0)
            copies[i, stage + 1] = copy(i, stage + 1)
            copies[i, stage + 1].start()
            lax.fori_loop(0, 1 << len(others), stay, 0)
    if tail:
        cells, tiles, _ = out_ref.shape
        mean = [total_ref[pl.ds(t * cells, cells), :] for t in range(tiles)]
        coupled = jnp.dot(
            coupling_ref[...], jnp.concatenate(mean, axis=1),
            precision=lax.Precision.HIGHEST, preferred_element_type=jnp.float32,
        )
        for t in range(tiles):
            out_ref[:, t, :] = sigma_ref[pl.ds(t, 1), :] * (mean[t] + coupled[:, t * width : (t + 1) * width])
    else:
        out_ref[...] = total_ref[...]
    for made in copies.values():
        made.wait_send()


def local_sums(
    innovations, block_owner, block_tile, block_count, obs_row, obs_col, offsets, obs_mask, tile_local, cells, peers
):
    blocks, obs, width = innovations.shape
    half, rows = peers // 2, tile_local * cells
    kind = jnp.float32 if peers * rows * width <= 1 << 22 else jnp.bfloat16
    smem = pl.BlockSpec(memory_space=pltpu.SMEM)
    vmem = pl.BlockSpec(memory_space=pltpu.VMEM)
    hbm = pl.BlockSpec(memory_space=pltpu.HBM)
    return pl.pallas_call(
        functools.partial(partial_kernel, cells),
        out_shape=(
            pltpu.VMEM((half, rows, width), jnp.bfloat16),
            pltpu.VMEM((half * rows, width), kind),
        ),
        in_specs=[smem] * 2 + [hbm, hbm] + [vmem] * 4,
        out_specs=(vmem, vmem),
        scratch_shapes=[
            pltpu.VMEM((2 * half * rows, width), jnp.float32),
            pltpu.VMEM((blocks, obs, width), jnp.bfloat16),
            pltpu.SMEM((1,), jnp.int32),
            pltpu.VMEM((blocks, obs), jnp.int32),
            pltpu.VMEM((4, blocks, obs), jnp.float32),
            pltpu.SemaphoreType.DMA,
            pltpu.SemaphoreType.DMA,
        ],
        compiler_params=pltpu.CompilerParams(vmem_limit_bytes=limit(peers, rows, width, -3, 62)),
    )(block_owner, block_tile, block_count, innovations, obs_row, obs_col, offsets, obs_mask)


def limit(peers, rows, width, whole, more):
    return peers * rows * width * whole + (more << 20)


def scatter_sums(send, keep, sigma, coupling, tile_local, cells, peers, tail):
    bits = peers.bit_length() - 1
    width, rows = sigma.shape[1], tile_local * cells
    streams = plans(bits, rows)
    vmem = pl.BlockSpec(memory_space=pltpu.VMEM)

    def room(first, kind):
        return [
            pltpu.VMEM((1 << (bits - 1 - stage), high - low, width), kind)
            for low, high, _ in streams
            for stage in range(first, bits)
        ]

    kept = [pltpu.VMEM((1 << (bits - 2), high - low, width), jnp.float32) for low, high, _ in streams]
    shape = (cells, tile_local, width) if tail else (rows, width)
    return pl.pallas_call(
        functools.partial(scatter_kernel, bits, streams, tail),
        out_shape=jax.ShapeDtypeStruct(shape, jnp.float32),
        in_specs=[vmem] * (4 if tail else 2),
        out_specs=vmem,
        scratch_shapes=room(0, jnp.bfloat16)
        + room(1, jnp.bfloat16)
        + kept
        + [
            pltpu.VMEM((rows, width), jnp.float32),
            pltpu.SemaphoreType.DMA((len(streams) * bits,)),
            pltpu.SemaphoreType.DMA((len(streams) * bits,)),
        ],
        compiler_params=pltpu.CompilerParams(
            collective_id=0, has_side_effects=True, vmem_limit_bytes=limit(peers, rows, width, 4, 4)
        ),
    )(send, keep, *((sigma, coupling) if tail else ()))


def on_device(
    innovations, block_owner, block_tile, block_count, obs_row, obs_col, offsets, obs_mask, sigma, coupling
):
    peers = lax.axis_size("space")
    ens_count = lax.axis_size("ens")
    members = ens_count * innovations.shape[0]
    tile_local, width = sigma.shape
    cells = coupling.shape[0]
    values = innovations[0]
    send, keep = local_sums(
        values, block_owner[:, 0], block_tile, block_count, obs_row, obs_col, offsets, obs_mask,
        tile_local, cells, peers,
    )
    totals = scatter_sums(send, keep, sigma, coupling, tile_local, cells, peers, members == 1)
    if members == 1:
        return totals
    totals = totals.reshape(tile_local, cells, width)
    share = cells // ens_count
    if ens_count > 1:
        totals = lax.psum(totals.astype(jnp.bfloat16), "ens").astype(jnp.float32)
    first = lax.axis_index("ens") * share
    coupling_rows = lax.dynamic_slice_in_dim(coupling, first, share, 0)
    own = lax.dynamic_slice_in_dim(totals, first, share, 1)
    coupled = jnp.einsum("ck,tkh->cth", coupling_rows, totals, precision=lax.Precision.HIGHEST)
    return sigma[None, :, :] * (jnp.transpose(own, (1, 0, 2)) + coupled) / members


def solution(mesh):
    in_specs = (
        P("ens", "space", None, None),
        P("space", None),
        P("space"),
        P("space"),
        P("space", None),
        P("space", None),
        P("space", None, None),
        P("space", None),
        P("space", None),
        P(),
    )
    out_specs = P("ens", "space", None)
    return jax.shard_map(
        on_device, mesh=mesh, in_specs=in_specs, out_specs=out_specs, check_vma=False
    )
```
